128 devices in a mesh: dom: 64 (over z_hi, x, y, core), grp: 2 (over z_lo).
Axes of the slice: x: 4, y: 4, z: 4 (z_hi: 2, z_lo: 2; z = z_hi * 2 + z_lo), core: 2. Of those that a mesh axis runs over, the one named last changes fastest.
Arguments:
- node_features: bfloat16 [1048576, 256], P(('dom', 'grp')), may hold values from -6 to 6
- vertex_count: int32 [128], P(('dom', 'grp')), may hold values from 4096 to 8192, as said below
- send_rows: int32 [128, 2, 2048], P(('dom', 'grp')), may hold values from 0 to 8191, as said below
- block_values: bfloat16 [8192, 4, 128, 128], P(('dom', 'grp')), may hold values from -0.25 to 0.25
- block_cols: int32 [8192, 4], P(('dom', 'grp')), may hold values from 0 to 95
- block_count: int32 [8192], P(('dom', 'grp')), may hold values from 1 to 4
- w_query: bfloat16 [2, 256, 256], replicated, may hold values from -0.375 to 0.375
- w_key: bfloat16 [2, 256, 256], replicated, may hold values from -0.375 to 0.375
- w_value: bfloat16 [2, 256, 256], replicated, may hold values from -0.375 to 0.375
- w_message: bfloat16 [2, 256, 256], replicated, may hold values from -0.375 to 0.375
- w_out: bfloat16 [2, 256, 256], replicated, may hold values from -0.375 to 0.375
- attn_gain: float32 [2, 256], replicated, may hold values from 0.25 to 1.75
Outputs:
- updated: bfloat16 [1048576, 256], P(('dom', 'grp'))
The draws below stay inside these ranges and needn't reach their ends.
Inputs may be any that keep to these rules, and one draw needn't show every extreme that they name: Rows of partition p at local index vertex_count[p] or above are padding; some partition uses all 8192 slots. send_rows[p, 0, :] and send_rows[p, 1, :] each list 2048 distinct local rows of partition p below vertex_count[p]. `block_cols`: extended tiles below 64 are the partition's own; the next 16 come from the lower neighbour, the last 16 from the upper one. Only the first block_count[g] blocks of row tile g are used.
All inputs are finite; a program needn't handle non-finite values.
Results may differ from the reference program's by a relative error of at most 0.0063.
Values may be sent and summed in bfloat16 or wider, within the bound.
A program may use at most 128 MiB of HBM per device.

```python
import jax
import jax.numpy as jnp
from jax import lax

D = 256
TILE = 128
NB = 4
LAYERS = 2
V_DEV = 8192
HALO = 2048
TILES_DEV = 64
EXT_TILES = 96
PARTITIONS = 128
VERTICES = 1048576
ALL_TILES = 8192


def count_draw(key):
    counts = jax.random.randint(jax.random.fold_in(key, 11), (PARTITIONS,), V_DEV // 2, V_DEV + 1)
    chosen = jax.random.randint(jax.random.fold_in(key, 12), (), 0, PARTITIONS)
    counts = jnp.where(jnp.arange(PARTITIONS) == chosen, V_DEV, counts)
    return counts.astype(jnp.int32)


def draw_vertex_count(key, part):
    return count_draw(key)


def draw_send_rows(key, part):
    counts = count_draw(key)
    scores = jax.random.randint(jax.random.fold_in(key, 13), (PARTITIONS, 2, V_DEV), 0, 1048576)
    row_index = jnp.arange(V_DEV, dtype=jnp.int32)
    beyond = row_index[None, None, :] >= counts[:, None, None]
    scores = scores + jnp.where(beyond, 2097152, 0)
    order = jnp.argsort(scores, axis=-1, stable=True)
    return order[:, :, :HALO].astype(jnp.int32)


def with_ends(drawn, key, smallest, top_value):
    index_at = [jax.random.randint(jax.random.fold_in(key, axis), (), 0, length) for axis, length in enumerate(drawn.shape)]
    widest = drawn.shape.index(max(drawn.shape))
    next_to = index_at[:widest] + [(index_at[widest] + 1) % drawn.shape[widest]] + index_at[widest + 1:]
    return drawn.at[tuple(index_at)].set(smallest).at[tuple(next_to)].set(top_value)


def block_scale(rng, shape, pieces, low, largest):
    gain = 1.0
    for dim, shards_of in pieces:
        draws = jax.random.uniform(jax.random.fold_in(jax.random.fold_in(rng, 6), dim), (shards_of,), jnp.float32, low / len(pieces), largest / len(pieces))
        gain = gain * jnp.repeat(jnp.exp(draws), shape[dim] // shards_of).reshape((-1,) + (1,) * (len(shape) - 1 - dim))
    return gain


def centred(own_key, shape, scale, most, split=(), held_as=jnp.bfloat16):
    drawn = scale * jax.random.normal(own_key, shape, jnp.float32)
    if split:
        drawn = drawn * block_scale(own_key, shape, split, -0.22, 0.18)
    return jnp.clip(drawn, -most, most).astype(held_as)


def setup_inputs(seed: int = 0) -> dict:
    splits = jax.random.split(jax.random.key(seed), 13)
    node_features = centred(splits[0], (VERTICES, D), 1.0, 6.0, ((0, 128),))
    vertex_count = draw_vertex_count(jax.random.fold_in(splits[12], 71), 0)
    send_rows = draw_send_rows(jax.random.fold_in(splits[12], 71), 0)
    block_values = centred(splits[3], (ALL_TILES, NB, TILE, TILE), (NB * TILE) ** -0.5, 0.25, ((0, 128),))
    block_cols = with_ends(jax.random.randint(splits[4], (ALL_TILES, NB), 0, EXT_TILES), jax.random.fold_in(splits[4], 1), 0, EXT_TILES - 1).astype(jnp.int32)
    block_count = with_ends(jax.random.randint(splits[5], (ALL_TILES,), 1, NB + 1), jax.random.fold_in(splits[5], 1), 1, NB).astype(jnp.int32)
    w_query = centred(splits[6], (LAYERS, D, D), D ** -0.5, 0.375)
    w_key = centred(splits[7], (LAYERS, D, D), D ** -0.5, 0.375)
    w_value = centred(splits[8], (LAYERS, D, D), D ** -0.5, 0.375)
    w_message = centred(splits[9], (LAYERS, D, D), D ** -0.5, 0.375)
    w_out = centred(splits[10], (LAYERS, D, D), D ** -0.5, 0.375)
    attn_gain = jnp.clip(1.0 + 0.15 * jax.random.normal(splits[11], (LAYERS, D), jnp.float32), 0.25, 1.75)
    return dict(node_features=node_features, vertex_count=vertex_count, send_rows=send_rows, block_values=block_values, block_cols=block_cols, block_count=block_count, w_query=w_query, w_key=w_key, w_value=w_value, w_message=w_message, w_out=w_out, attn_gain=attn_gain)


epsilon = 1e-06

def feature_map(inputs):
    return jax.nn.elu(inputs) + 1.0

def reference(node_features, vertex_count, send_rows, block_values, block_cols, block_count, w_query, w_key, w_value, w_message, w_out, attn_gain):
    row_index = jnp.arange(V_DEV, dtype=jnp.int32)
    valid_rows = (row_index[None, :] < vertex_count[:, None]).astype(jnp.float32)
    hidden = node_features.reshape(PARTITIONS, V_DEV, D)
    hidden = jnp.where(valid_rows[..., None] > 0.5, hidden, jnp.zeros_like(hidden))
    tile_blocks = block_values.reshape(PARTITIONS, TILES_DEV, NB, TILE, TILE)
    tile_cols = block_cols.reshape(PARTITIONS, TILES_DEV, NB)
    tile_counts = block_count.reshape(PARTITIONS, TILES_DEV)
    for layer_num in range(LAYERS):

        def add_summary(running, entries):
            part_rows, keep_rows = entries
            key_rows = (feature_map(jnp.dot(part_rows, w_key[layer_num], preferred_element_type=jnp.float32)) * keep_rows[:, None]).astype(jnp.bfloat16)
            value_rows = jnp.dot(part_rows, w_value[layer_num], preferred_element_type=jnp.float32).astype(jnp.bfloat16)
            return (running + jnp.dot(key_rows.T, value_rows, preferred_element_type=jnp.float32), None)
        summary, _ = lax.scan(add_summary, jnp.zeros((D, D), jnp.float32), (hidden, valid_rows))
        summary_cast = summary.astype(jnp.bfloat16)
        outgoing = jax.vmap(lambda part_rows, row_list: part_rows[row_list])(hidden, send_rows)
        zero_rows = jnp.zeros((1, HALO, D), jnp.bfloat16)
        lower_rows = jnp.concatenate([zero_rows, outgoing[:-1, 1]], axis=0)
        upper_rows = jnp.concatenate([outgoing[1:, 0], zero_rows], axis=0)

        def update(entries):
            part_rows, keep_rows, below, above, blocks_here, cols_here, counts_here = entries
            extended = jnp.concatenate([part_rows, below, above], axis=0).reshape(EXT_TILES, TILE, D)
            picked = extended[cols_here]
            live_slots = jnp.arange(NB, dtype=jnp.int32)[None, :] < counts_here[:, None]
            used_blocks = jnp.where(live_slots[:, :, None, None], blocks_here, jnp.zeros_like(blocks_here))
            aggregated = jnp.einsum('tjab,tjbd->tad', used_blocks.astype(jnp.float32), picked.astype(jnp.float32))
            aggregated = aggregated.reshape(V_DEV, D).astype(jnp.bfloat16)
            message = jax.nn.silu(jnp.dot(aggregated, w_message[layer_num], preferred_element_type=jnp.float32))
            query_rows = feature_map(jnp.dot(part_rows, w_query[layer_num], preferred_element_type=jnp.float32)).astype(jnp.bfloat16)
            mixed_rows = jnp.dot(query_rows, summary_cast, preferred_element_type=jnp.float32)
            scale = lax.rsqrt(lax.optimization_barrier(jnp.mean(mixed_rows * mixed_rows, axis=-1, keepdims=True)) + epsilon)
            attended = (mixed_rows * scale * attn_gain[layer_num][None, :]).astype(jnp.bfloat16)
            output = jnp.dot(attended, w_out[layer_num], preferred_element_type=jnp.float32)
            renewed = part_rows.astype(jnp.float32) + message + output
            renewed = jnp.where(keep_rows[:, None] > 0.5, renewed, jnp.zeros_like(renewed))
            return renewed.astype(jnp.bfloat16)
        hidden = lax.map(update, (hidden, valid_rows, lower_rows, upper_rows, tile_blocks, tile_cols, tile_counts))
    return hidden.reshape(VERTICES, D)
```

```python
import functools

import jax
import jax.numpy as jnp
from jax import lax
from jax.experimental import pallas as pl
from jax.experimental.pallas import tpu as pltpu
from jax.sharding import PartitionSpec as P

MESH = pl.DeviceIdType.MESH
epsilon = 1e-06
F32 = jnp.float32
BF16 = jnp.bfloat16

NX, NY, NZ = 4, 4, 4
ROWS = 512
UNROLL = 16
FIRST = 8


def repeat(start, stop, body):
    def step(i, carry):
        body(i)
        return carry

    lax.fori_loop(start, stop, step, 0)


def feature_map(u):
    return jnp.maximum(u, 0.0) + jnp.exp(jnp.minimum(u, 0.0))


def silu(u):
    return 0.5 * u * (1.0 + jnp.tanh(0.5 * u))


def dot(a, b):
    return jnp.dot(a, b, preferred_element_type=F32)


def kernel(
    sizes,
    count_ref,
    rows_ref,
    near_ref,
    far_ref,
    feat_ref,
    blocks_ref,
    wq_ref,
    wk_ref,
    wv_ref,
    wm_ref,
    wo_ref,
    gain_ref,
    out_ref,
    hid,
    halo_0,
    halo_1,
    wide,
    picked,
    send,
    query,
    local,
    res,
    blk,
    summ,
    half,
    quarter,
    piece,
    r1,
    r2,
    r3,
    r4,
    total,
    feat_sem,
    blk_sem,
    out_sem,
    halo_send,
    halo_recv,
    ar_send,
    ar_recv,
):
    layers, vertices, width, tile, slots, halo_rows = sizes
    halos = (halo_0, halo_1)
    tiles = vertices // tile
    side_tiles = halo_rows // tile
    lanes = width // 2
    steps = vertices // ROWS

    dom, grp = lax.axis_index("dom"), lax.axis_index("grp")
    part = dom * 2 + grp
    parts = NX * NY * NZ * 2
    core = lax.rem(dom, 2)
    y = lax.rem(dom // 2, NY)
    x = lax.rem(dom // (2 * NY), NX)
    z = dom // (2 * NY * NX) * 2 + grp

    def place(x_at, y_at, z_at, core_at):
        return {
            "dom": ((z_at // 2 * NX + x_at) * NY + y_at) * 2 + core_at,
            "grp": lax.rem(z_at, 2),
        }

    def place_of(part_at):
        return {"dom": part_at // 2, "grp": lax.rem(part_at, 2)}

    upper = place_of(lax.rem(part + 1, parts))
    lower = place_of(lax.rem(part + parts - 1, parts))
    twin = place(x, y, z, 1 - core)
    x_others = [place(lax.rem(x + k, NX), y, z, core) for k in range(1, NX)]
    y_others = [place(x, lax.rem(y + k, NY), z, core) for k in range(1, NY)]
    z_others = [place(x, y, lax.rem(z + k, NZ), core) for k in range(1, NZ)]

    some_tiles = ROWS // tile

    def hidden(i):
        return hid[pl.ds(i * some_tiles, some_tiles)].reshape(ROWS, width)

    def set_hidden(i, new):
        hid[pl.ds(i * some_tiles, some_tiles)] = new.reshape(some_tiles, tile, width)

    def feat_copy(i):
        at = pl.ds(i * some_tiles, some_tiles)
        return pltpu.make_async_copy(feat_ref.at[at], hid.at[at], feat_sem.at[i])

    def blk_copy(i):
        return pltpu.make_async_copy(blocks_ref.at[i], blk.at[i], blk_sem.at[i])

    for i in range(steps):
        feat_copy(i).start()

    barrier = pltpu.get_barrier_semaphore()
    partners = [upper, lower, twin] + x_others + y_others + z_others
    for partner in partners:
        pl.semaphore_signal(barrier, inc=1, device_id=partner, device_id_type=MESH)

    count = count_ref[0]
    hid[tiles] = jnp.zeros((tile, width), BF16)
    for halo in halos:
        halo[2 * side_tiles] = jnp.zeros((tile, width), BF16)

    def keep(i):
        at = i * ROWS + lax.broadcasted_iota(jnp.int32, (ROWS, width), 0)
        return at < count

    def widen(i, new):
        wide[pl.ds(2 * i * ROWS, ROWS, stride=2), :] = new[:, :lanes]
        wide[pl.ds(2 * i * ROWS + 1, ROWS, stride=2), :] = new[:, lanes:]

    def enter(i):
        feat_copy(i).wait()
        kept = jnp.where(keep(i), hidden(i).astype(F32), 0.0)
        set_hidden(i, kept.astype(BF16))
        widen(i, kept)

    repeat(0, steps, enter)
    repeat(0, tiles, lambda i: blk_copy(i).start())
    pl.semaphore_wait(barrier, len(partners))

    def halo_copy(layer, side, k):
        at = (1 - side) * side_tiles
        return pltpu.make_async_remote_copy(
            src_ref=send.at[side, k],
            dst_ref=halos[layer].at[at + k],
            send_sem=halo_send.at[side, k],
            recv_sem=halo_recv.at[layer, side, k],
            device_id=lower if side == 0 else upper,
            device_id_type=MESH,
        )

    def gather(layer, first, last):
        def chunk(k):
            for side in range(2):
                def some(i):
                    for u in range(UNROLL):
                        at = i * UNROLL + u
                        row = rows_ref[side, k * tile + at]
                        picked[side, pl.ds(2 * at, 2), :] = wide[pl.ds(2 * row, 2), :]

                repeat(0, tile // UNROLL, some)
                send[side, k, :, :lanes] = picked[side, pl.ds(0, tile, stride=2), :].astype(BF16)
                send[side, k, :, lanes:] = picked[side, pl.ds(1, tile, stride=2), :].astype(BF16)
            for side in range(2):
                halo_copy(layer, side, k).start()

        repeat(first, last, chunk)

    def exchange(layer, number, src, dst, target):
        return pltpu.make_async_remote_copy(
            src_ref=src,
            dst_ref=dst,
            send_sem=ar_send.at[layer, number],
            recv_sem=ar_recv.at[layer, number],
            device_id=target,
            device_id_type=MESH,
        )

    def start(copies):
        for copy in copies:
            copy.start()

    def wait(copies):
        for copy in copies:
            copy.wait()

    def blocks_of(t):
        return jnp.concatenate([blk[t, j] for j in range(slots)], axis=1)

    for layer in range(layers):
        wk_t = wk_ref[layer].T
        wv, wq = wv_ref[layer], wq_ref[layer]

        gather(layer, 0, FIRST)

        summ[...] = jnp.zeros_like(summ)

        def add_summary(i):
            h = hidden(i)
            keys = lax.dot_general(wk_t, h, (((1,), (1,)), ((), ())), preferred_element_type=F32)
            keys = feature_map(keys).astype(BF16)
            values = dot(h, wv).astype(BF16)
            summ[...] += dot(keys, values)

        repeat(0, steps, add_summary)

        def ask(i):
            rows = pl.ds(i * ROWS, ROWS)
            query[rows, :] = feature_map(dot(hidden(i), wq)).astype(BF16)

        group = 4

        def gather_local(i):
            for u in range(group):
                t = i * group + u
                if layer == 0:
                    blk_copy(t).wait()
                tiles_here = [hid[near_ref[t * slots + j]] for j in range(slots)]
                local[pl.ds(t * tile, tile), :] = dot(
                    blocks_of(t), jnp.concatenate(tiles_here, axis=0)
                )

        loops = tiles // group

        share = width // 2
        hop = [
            exchange(layer, 0, summ.at[pl.ds((1 - core) * share, share)], r1.at[layer], twin)
        ]
        start(hop)
        repeat(0, steps // 2, ask)
        wait(hop)
        half[...] = summ[pl.ds(core * share, share), :] + r1[layer]

        share //= NX
        hop = [
            exchange(
                layer,
                k,
                half.at[pl.ds(lax.rem(x + k, NX) * share, share)],
                r2.at[layer, k - 1],
                x_others[k - 1],
            )
            for k in range(1, NX)
        ]
        start(hop)
        repeat(steps // 2, steps, ask)
        wait(hop)
        quarter[...] = half[pl.ds(x * share, share), :] + (
            r2[layer, 0] + r2[layer, 1] + r2[layer, 2]
        )

        share //= NY
        hop = [
            exchange(
                layer,
                k + 3,
                quarter.at[pl.ds(lax.rem(y + k, NY) * share, share)],
                r3.at[layer, k - 1],
                y_others[k - 1],
            )
            for k in range(1, NY)
        ]
        start(hop)
        repeat(0, loops // 4, gather_local)
        wait(hop)
        piece[...] = quarter[pl.ds(y * share, share), :] + (
            r3[layer, 0] + r3[layer, 1] + r3[layer, 2]
        )

        hop = [
            exchange(layer, k + 6, piece, r4.at[layer, k - 1], z_others[k - 1])
            for k in range(1, NZ)
        ]
        start(hop)
        gather(layer, FIRST, side_tiles)
        repeat(loops // 4, loops // 2, gather_local)
        wait(hop)
        at = core * (width // 2) + x * (width // 8) + y * share
        total[layer, pl.ds(at, share), :] = piece[...] + (
            r4[layer, 0] + r4[layer, 1] + r4[layer, 2]
        )

        here = total.at[layer, pl.ds(at, share)]
        hop = [
            exchange(layer, k + 9, here, here, y_others[k - 1]) for k in range(1, NY)
        ]
        start(hop)
        repeat(loops // 2, loops // 4 * 3, gather_local)
        wait(hop)
        here = total.at[layer, pl.ds(core * (width // 2) + x * (width // 8), width // 8)]
        hop = [
            exchange(layer, k + 12, here, here, x_others[k - 1]) for k in range(1, NX)
        ]
        start(hop)
        repeat(loops // 4 * 3, loops, gather_local)
        wait(hop)
        here = total.at[layer, pl.ds(core * (width // 2), width // 2)]
        hop = [exchange(layer, 16, here, here, twin)]
        start(hop)
        wait(hop)
        summary = total[layer].astype(BF16)
        wo, wm = wo_ref[layer], wm_ref[layer]
        gain = gain_ref[pl.ds(layer, 1), :]

        def attend(i):
            rows = pl.ds(i * ROWS, ROWS)
            mixed = dot(query[rows, :], summary)
            scale = lax.rsqrt(jnp.mean(mixed * mixed, axis=-1, keepdims=True) + epsilon)
            attended = (mixed * scale * gain).astype(BF16)
            res[rows, :] = hidden(i).astype(F32) + dot(attended, wo)

        repeat(0, steps, attend)

        def arrived(k):
            for side in range(2):
                halo_copy(layer, side, k).wait()

        repeat(0, side_tiles, arrived)

        def out_copy(i):
            at = pl.ds(i * some_tiles, some_tiles)
            return pltpu.make_async_copy(hid.at[at], out_ref.at[at], out_sem.at[i])

        def finish(i):
            for u in range(some_tiles):
                t = i * some_tiles + u
                tiles_here = [halos[layer][far_ref[t * slots + j]] for j in range(slots)]
                rows = pl.ds(t * tile, tile)
                local[rows, :] += dot(blocks_of(t), jnp.concatenate(tiles_here, axis=0))
            rows = pl.ds(i * ROWS, ROWS)
            message = silu(dot(local[rows, :].astype(BF16), wm))
            new = jnp.where(keep(i), res[rows, :] + message, 0.0).astype(BF16)
            set_hidden(i, new)
            if layer < layers - 1:
                widen(i, new.astype(F32))
            else:
                out_copy(i).start()

        repeat(0, steps, finish)
        if layer == layers - 1:
            repeat(0, steps, lambda i: out_copy(i).wait())


def on_device(
    node_features,
    vertex_count,
    send_rows,
    block_values,
    block_cols,
    block_count,
    w_query,
    w_key,
    w_value,
    w_message,
    w_out,
    attn_gain,
):
    vertices, width = node_features.shape
    tiles, slots, tile, _ = block_values.shape
    layers = w_query.shape[0]
    halo_rows = send_rows.shape[2]
    side_tiles = halo_rows // tile
    steps = vertices // ROWS
    smem = pl.BlockSpec(memory_space=pltpu.SMEM)
    vmem = pl.BlockSpec(memory_space=pltpu.VMEM)
    anywhere = pl.BlockSpec(memory_space=pl.ANY)
    hops = 17

    part = lax.axis_index(("dom", "grp"))
    parts = lax.axis_size(("dom", "grp"))
    live = jnp.arange(slots, dtype=jnp.int32)[None, :] < block_count[:, None]
    near = jnp.where(live & (block_cols < tiles), block_cols, tiles)
    first = tiles + jnp.where(part > 0, 0, side_tiles)
    last = tiles + jnp.where(part < parts - 1, 2 * side_tiles, side_tiles)
    far = jnp.where(live & (block_cols >= first) & (block_cols < last), block_cols - tiles, 2 * side_tiles)
    out = pl.pallas_call(
        functools.partial(kernel, (layers, vertices, width, tile, slots, halo_rows)),
        out_shape=jax.ShapeDtypeStruct((tiles, tile, width), BF16),
        in_specs=[smem] * 4 + [anywhere] * 2 + [vmem] * 6,
        out_specs=anywhere,
        scratch_shapes=[
            pltpu.VMEM((tiles + 1, tile, width), BF16),
            pltpu.VMEM((2 * side_tiles + 1, tile, width), BF16),
            pltpu.VMEM((2 * side_tiles + 1, tile, width), BF16),
            pltpu.VMEM((2 * vertices, width // 2), F32),
            pltpu.VMEM((2, 2 * tile, width // 2), F32),
            pltpu.VMEM((2, side_tiles, tile, width), BF16),
            pltpu.VMEM((vertices, width), BF16),
            pltpu.VMEM((vertices, width), F32),
            pltpu.VMEM((vertices, width), F32),
            pltpu.VMEM((tiles, slots, tile, tile), BF16),
            pltpu.VMEM((width, width), F32),
            pltpu.VMEM((width // 2, width), F32),
            pltpu.VMEM((width // 8, width), F32),
            pltpu.VMEM((width // 32, width), F32),
            pltpu.VMEM((layers, width // 2, width), F32),
            pltpu.VMEM((layers, 3, width // 8, width), F32),
            pltpu.VMEM((layers, 3, width // 32, width), F32),
            pltpu.VMEM((layers, 3, width // 32, width), F32),
            pltpu.VMEM((layers, width, width), F32),
            pltpu.SemaphoreType.DMA((steps,)),
            pltpu.SemaphoreType.DMA((tiles,)),
            pltpu.SemaphoreType.DMA((steps,)),
            pltpu.SemaphoreType.DMA((2, side_tiles)),
            pltpu.SemaphoreType.DMA((layers, 2, side_tiles)),
            pltpu.SemaphoreType.DMA((layers, hops)),
            pltpu.SemaphoreType.DMA((layers, hops)),
        ],
        compiler_params=pltpu.CompilerParams(
            collective_id=0, has_side_effects=True, vmem_limit_bytes=67043328
        ),
        name="graph_layers",
    )(
        vertex_count,
        send_rows[0],
        near.reshape(-1),
        far.reshape(-1),
        node_features.reshape(tiles, tile, width),
        block_values,
        w_query,
        w_key,
        w_value,
        w_message,
        w_out,
        attn_gain,
    )
    return out.reshape(vertices, width)


def solution(mesh):
    placed = (
        P(("dom", "grp"), None),
        P(("dom", "grp")),
        P(("dom", "grp"), None, None),
        P(("dom", "grp"), None, None, None),
        P(("dom", "grp"), None),
        P(("dom", "grp")),
        P(),
        P(),
        P(),
        P(),
        P(),
        P(),
    )
    return jax.shard_map(
        on_device, mesh=mesh, in_specs=placed, out_specs=P(("dom", "grp"), None), check_vma=False
    )
```

```python
import functools

import jax
import jax.numpy as jnp
from jax import lax
from jax.experimental import pallas as pl
from jax.experimental.pallas import tpu as pltpu
from jax.sharding import PartitionSpec as P

MESH = pl.DeviceIdType.MESH
epsilon = 1e-06
F32 = jnp.float32
BF16 = jnp.bfloat16

NX, NY, NZ = 4, 4, 4
ROWS = 512
UNROLL = 32
BLOCK_COPIES = 4
FIRST = 8


def repeat(start, stop, body):
    def step(i, carry):
        body(i)
        return carry

    lax.fori_loop(start, stop, step, 0)


def feature_map(u):
    return jnp.maximum(u, 0.0) + jnp.exp(jnp.minimum(u, 0.0))


def silu(u):
    return 0.5 * u * (1.0 + jnp.tanh(0.5 * u))


def dot(a, b):
    return jnp.dot(a, b, preferred_element_type=F32)


def kernel(
    sizes,
    count_ref,
    rows_ref,
    cols_ref,
    used_ref,
    feat_ref,
    blocks_ref,
    wq_ref,
    wk_ref,
    wv_ref,
    wm_ref,
    wo_ref,
    gain_ref,
    out_ref,
    hid,
    halo_0,
    halo_1,
    wide,
    picked,
    send,
    query,
    local,
    res,
    blk,
    summ,
    half,
    quarter,
    piece,
    r1,
    r2,
    r3,
    r4,
    total,
    near_ref,
    far_ref,
    feat_sem,
    blk_sem,
    halo_send,
    halo_recv,
    ar_send,
    ar_recv,
):
    layers, vertices, width, tile, slots, halo_rows = sizes
    halos = (halo_0, halo_1)
    tiles = vertices // tile
    side_tiles = halo_rows // tile
    lanes = width // 2
    steps = vertices // ROWS

    dom, grp = lax.axis_index("dom"), lax.axis_index("grp")
    part = dom * 2 + grp
    parts = NX * NY * NZ * 2
    core = lax.rem(dom, 2)
    y = lax.rem(dom // 2, NY)
    x = lax.rem(dom // (2 * NY), NX)
    z = dom // (2 * NY * NX) * 2 + grp

    def place(x_at, y_at, z_at, core_at):
        return {
            "dom": ((z_at // 2 * NX + x_at) * NY + y_at) * 2 + core_at,
            "grp": lax.rem(z_at, 2),
        }

    def place_of(part_at):
        return {"dom": part_at // 2, "grp": lax.rem(part_at, 2)}

    upper = place_of(lax.rem(part + 1, parts))
    lower = place_of(lax.rem(part + parts - 1, parts))
    twin = place(x, y, z, 1 - core)
    x_others = [place(lax.rem(x + k, NX), y, z, core) for k in range(1, NX)]
    y_others = [place(x, lax.rem(y + k, NY), z, core) for k in range(1, NY)]
    z_others = [place(x, y, lax.rem(z + k, NZ), core) for k in range(1, NZ)]

    some_tiles = ROWS // tile

    def hidden(i):
        return hid[pl.ds(i * some_tiles, some_tiles)].reshape(ROWS, width)

    def set_hidden(i, new):
        hid[pl.ds(i * some_tiles, some_tiles)] = new.reshape(some_tiles, tile, width)

    def feat_copy(i):
        at = pl.ds(i * some_tiles, some_tiles)
        return pltpu.make_async_copy(feat_ref.at[at], hid.at[at], feat_sem.at[i])

    def blk_copy(i):
        at = pl.ds(i * (tiles // BLOCK_COPIES), tiles // BLOCK_COPIES)
        return pltpu.make_async_copy(blocks_ref.at[at], blk.at[at], blk_sem.at[i])

    for i in range(steps):
        feat_copy(i).start()

    barrier = pltpu.get_barrier_semaphore()
    partners = [upper, lower, twin] + x_others + y_others + z_others
    for partner in partners:
        pl.semaphore_signal(barrier, inc=1, device_id=partner, device_id_type=MESH)

    count = count_ref[0]
    hid[tiles] = jnp.zeros((tile, width), BF16)
    for halo in halos:
        halo[2 * side_tiles] = jnp.zeros((tile, width), BF16)

    def keep(i, new):
        at = i * ROWS + lax.broadcasted_iota(jnp.int32, (ROWS, lanes), 0)
        used = at < count
        return jnp.concatenate(
            [jnp.where(used, new[:, :lanes], 0.0), jnp.where(used, new[:, lanes:], 0.0)], axis=1
        )

    def widen(i, new):
        wide[pl.ds(2 * i * ROWS, ROWS, stride=2), :] = new[:, :lanes]
        wide[pl.ds(2 * i * ROWS + 1, ROWS, stride=2), :] = new[:, lanes:]

    def enter(i):
        feat_copy(i).wait()
        kept = keep(i, hidden(i).astype(F32))
        set_hidden(i, kept.astype(BF16))
        widen(i, kept)

    repeat(0, steps, enter)
    for i in range(BLOCK_COPIES):
        blk_copy(i).start()
    pl.semaphore_wait(barrier, len(partners))

    def halo_copy(layer, side, k):
        at = (1 - side) * side_tiles
        return pltpu.make_async_remote_copy(
            src_ref=send.at[side, k],
            dst_ref=halos[layer].at[at + k],
            send_sem=halo_send.at[side, k],
            recv_sem=halo_recv.at[layer, side, k],
            device_id=lower if side == 0 else upper,
            device_id_type=MESH,
        )

    def gather(layer, first, last):
        def chunk(k):
            for side in range(2):
                base = (2 * k + side) * tile

                def some(i):
                    at = i * UNROLL
                    some_rows = [rows_ref[base + at + u] for u in range(UNROLL)]
                    loaded = [wide[pl.ds(2 * row, 2), :] for row in some_rows]
                    for u in range(UNROLL):
                        picked[side, pl.ds(2 * (at + u), 2), :] = loaded[u]

                repeat(0, tile // UNROLL, some)
                send[side, k, :, :lanes] = picked[side, pl.ds(0, tile, stride=2), :].astype(BF16)
                send[side, k, :, lanes:] = picked[side, pl.ds(1, tile, stride=2), :].astype(BF16)
            for side in range(2):
                halo_copy(layer, side, k).start()

        repeat(first, last, chunk)

    def between(value, low, high):
        return jnp.minimum(jnp.maximum(value, low), high)

    first = tiles + side_tiles * between(1 - part, 0, 1)
    last = tiles + side_tiles * (1 + between(parts - 1 - part, 0, 1))

    def index(t):
        for j in range(slots):
            col = cols_ref[j, t]
            live = between(used_ref[t] - j, 0, 1)
            own = live * between(tiles - col, 0, 1)
            near_ref[t * slots + j] = tiles + (col - tiles) * own
            side = live * between(col - first + 1, 0, 1) * between(last - col, 0, 1)
            far_ref[t * slots + j] = 2 * side_tiles + (col - tiles - 2 * side_tiles) * side

    def exchange(layer, number, src, dst, target):
        return pltpu.make_async_remote_copy(
            src_ref=src,
            dst_ref=dst,
            send_sem=ar_send.at[layer, number],
            recv_sem=ar_recv.at[layer, number],
            device_id=target,
            device_id_type=MESH,
        )

    def start(copies):
        for copy in copies:
            copy.start()

    def wait(copies):
        for copy in copies:
            copy.wait()

    def blocks_of(t):
        return jnp.concatenate([blk[t, j] for j in range(slots)], axis=1)

    for layer in range(layers):
        wk_t = wk_ref[layer].T
        wv, wq = wv_ref[layer], wq_ref[layer]

        gather(layer, 0, FIRST)

        if layer == 0:
            repeat(0, tiles, index)
        summ[...] = jnp.zeros_like(summ)

        def add_summary(i):
            h = hidden(i)
            keys = lax.dot_general(wk_t, h, (((1,), (1,)), ((), ())), preferred_element_type=F32)
            keys = feature_map(keys).astype(BF16)
            values = dot(h, wv).astype(BF16)
            summ[...] += dot(keys, values)

        repeat(0, steps, add_summary)

        def ask(i):
            rows = pl.ds(i * ROWS, ROWS)
            query[rows, :] = feature_map(dot(hidden(i), wq)).astype(BF16)

        group = 4

        def gather_local(i):
            for u in range(group):
                t = i * group + u
                tiles_here = [hid[near_ref[t * slots + j]] for j in range(slots)]
                local[pl.ds(t * tile, tile), :] = dot(
                    blocks_of(t), jnp.concatenate(tiles_here, axis=0)
                )

        loops = tiles // group
        if layer == 0:
            for i in range(BLOCK_COPIES):
                blk_copy(i).wait()

        share = width // 2
        hop = [
            exchange(layer, 0, summ.at[pl.ds((1 - core) * share, share)], r1.at[layer], twin)
        ]
        start(hop)
        repeat(0, steps // 2, ask)
        wait(hop)
        half[...] = summ[pl.ds(core * share, share), :] + r1[layer]

        share //= NX
        hop = [
            exchange(
                layer,
                k,
                half.at[pl.ds(lax.rem(x + k, NX) * share, share)],
                r2.at[layer, k - 1],
                x_others[k - 1],
            )
            for k in range(1, NX)
        ]
        start(hop)
        repeat(steps // 2, steps, ask)
        wait(hop)
        quarter[...] = half[pl.ds(x * share, share), :] + (
            r2[layer, 0] + r2[layer, 1] + r2[layer, 2]
        )

        share //= NY
        hop = [
            exchange(
                layer,
                k + 3,
                quarter.at[pl.ds(lax.rem(y + k, NY) * share, share)],
                r3.at[layer, k - 1],
                y_others[k - 1],
            )
            for k in range(1, NY)
        ]
        start(hop)
        repeat(0, loops // 4, gather_local)
        wait(hop)
        piece[...] = quarter[pl.ds(y * share, share), :] + (
            r3[layer, 0] + r3[layer, 1] + r3[layer, 2]
        )

        hop = [
            exchange(layer, k + 6, piece, r4.at[layer, k - 1], z_others[k - 1])
            for k in range(1, NZ)
        ]
        start(hop)
        gather(layer, FIRST, side_tiles)
        repeat(loops // 4, loops // 2, gather_local)
        wait(hop)
        at = core * (width // 2) + x * (width // 8) + y * share
        total[layer, pl.ds(at, share), :] = piece[...] + (
            r4[layer, 0] + r4[layer, 1] + r4[layer, 2]
        )

        here = total.at[layer, pl.ds(at, share)]
        hop = [
            exchange(layer, k + 9, here, here, y_others[k - 1]) for k in range(1, NY)
        ]
        start(hop)
        repeat(loops // 2, loops // 4 * 3, gather_local)
        wait(hop)
        here = total.at[layer, pl.ds(core * (width // 2) + x * (width // 8), width // 8)]
        hop = [
            exchange(layer, k + 12, here, here, x_others[k - 1]) for k in range(1, NX)
        ]
        start(hop)
        repeat(loops // 4 * 3, loops, gather_local)
        wait(hop)
        here = total.at[layer, pl.ds(core * (width // 2), width // 2)]
        hop = [exchange(layer, 16, here, here, twin)]
        start(hop)
        wait(hop)
        summary = total[layer].astype(BF16)
        wo, wm = wo_ref[layer], wm_ref[layer]
        gain = gain_ref[pl.ds(layer, 1), :]

        def attend(i):
            rows = pl.ds(i * ROWS, ROWS)
            mixed = dot(query[rows, :], summary)
            scale = lax.rsqrt(jnp.mean(mixed * mixed, axis=-1, keepdims=True) + epsilon)
            attended = (mixed * scale * gain).astype(BF16)
            res[rows, :] = hidden(i).astype(F32) + dot(attended, wo)

        repeat(0, steps, attend)

        def arrived(k):
            for side in range(2):
                halo_copy(layer, side, k).wait()

        repeat(0, side_tiles, arrived)

        def finish(i):
            parts_here = []
            for u in range(some_tiles):
                t = i * some_tiles + u
                tiles_here = [halos[layer][far_ref[t * slots + j]] for j in range(slots)]
                both = local[pl.ds(t * tile, tile), :] + dot(
                    blocks_of(t), jnp.concatenate(tiles_here, axis=0)
                )
                parts_here.append(both.astype(BF16))
            message = silu(dot(jnp.concatenate(parts_here, axis=0), wm))
            new = keep(i, res[pl.ds(i * ROWS, ROWS), :] + message).astype(BF16)
            if layer < layers - 1:
                set_hidden(i, new)
                widen(i, new.astype(F32))
            else:
                out_ref[pl.ds(i * some_tiles, some_tiles)] = new.reshape(some_tiles, tile, width)

        repeat(0, steps, finish)


def on_device(
    node_features,
    vertex_count,
    send_rows,
    block_values,
    block_cols,
    block_count,
    w_query,
    w_key,
    w_value,
    w_message,
    w_out,
    attn_gain,
):
    vertices, width = node_features.shape
    tiles, slots, tile, _ = block_values.shape
    layers = w_query.shape[0]
    halo_rows = send_rows.shape[2]
    side_tiles = halo_rows // tile
    steps = vertices // ROWS
    smem = pl.BlockSpec(memory_space=pltpu.SMEM)
    vmem = pl.BlockSpec(memory_space=pltpu.VMEM)
    anywhere = pl.BlockSpec(memory_space=pl.ANY)
    hops = 17

    out = pl.pallas_call(
        functools.partial(kernel, (layers, vertices, width, tile, slots, halo_rows)),
        out_shape=pltpu.VMEM((tiles, tile, width), BF16),
        in_specs=[smem] * 4 + [anywhere] * 2 + [vmem] * 6,
        out_specs=vmem,
        scratch_shapes=[
            pltpu.VMEM((tiles + 1, tile, width), BF16),
            pltpu.VMEM((2 * side_tiles + 1, tile, width), BF16),
            pltpu.VMEM((2 * side_tiles + 1, tile, width), BF16),
            pltpu.VMEM((2 * vertices, width // 2), F32),
            pltpu.VMEM((2, 2 * tile, width // 2), F32),
            pltpu.VMEM((2, side_tiles, tile, width), BF16),
            pltpu.VMEM((vertices, width), BF16),
            pltpu.VMEM((vertices, width), F32),
            pltpu.VMEM((vertices, width), F32),
            pltpu.VMEM((tiles, slots, tile, tile), BF16),
            pltpu.VMEM((width, width), F32),
            pltpu.VMEM((width // 2, width), F32),
            pltpu.VMEM((width // 8, width), F32),
            pltpu.VMEM((width // 32, width), F32),
            pltpu.VMEM((layers, width // 2, width), F32),
            pltpu.VMEM((layers, 3, width // 8, width), F32),
            pltpu.VMEM((layers, 3, width // 32, width), F32),
            pltpu.VMEM((layers, 3, width // 32, width), F32),
            pltpu.VMEM((layers, width, width), F32),
            pltpu.SMEM((tiles * slots,), jnp.int32),
            pltpu.SMEM((tiles * slots,), jnp.int32),
            pltpu.SemaphoreType.DMA((steps,)),
            pltpu.SemaphoreType.DMA((BLOCK_COPIES,)),
            pltpu.SemaphoreType.DMA((2, side_tiles)),
            pltpu.SemaphoreType.DMA((layers, 2, side_tiles)),
            pltpu.SemaphoreType.DMA((layers, hops)),
            pltpu.SemaphoreType.DMA((layers, hops)),
        ],
        compiler_params=pltpu.CompilerParams(
            collective_id=0, has_side_effects=True, vmem_limit_bytes=58 * 2**20
        ),
        name="graph_layers",
    )(
        vertex_count,
        send_rows[0].reshape(2, side_tiles, tile).transpose(1, 0, 2).reshape(-1),
        block_cols.T,
        block_count,
        node_features.reshape(tiles, tile, width),
        block_values,
        w_query,
        w_key,
        w_value,
        w_message,
        w_out,
        attn_gain,
    )
    return out.reshape(vertices, width)


def solution(mesh):
    placed = (
        P(("dom", "grp"), None),
        P(("dom", "grp")),
        P(("dom", "grp"), None, None),
        P(("dom", "grp"), None, None, None),
        P(("dom", "grp"), None),
        P(("dom", "grp")),
        P(),
        P(),
        P(),
        P(),
        P(),
        P(),
    )
    return jax.shard_map(
        on_device, mesh=mesh, in_specs=placed, out_specs=P(("dom", "grp"), None), check_vma=False
    )
```

```python
import functools

import jax
import jax.numpy as jnp
from jax import lax
from jax.experimental import pallas as pl
from jax.experimental.pallas import tpu as pltpu
from jax.sharding import PartitionSpec as P

MESH = pl.DeviceIdType.MESH
epsilon = 1e-06
F32 = jnp.float32
BF16 = jnp.bfloat16

NX, NY, NZ = 4, 4, 4
ROWS = 4096
ENTRY_ROWS = 1024
GROUP = 16
UNROLL = 32
BLOCK_COPIES = 4
FIRST = 8


def repeat(start, stop, body):
    def step(i, carry):
        body(i)
        return carry

    lax.fori_loop(start, stop, step, 0)


def feature_map(u):
    return jnp.maximum(u, 0.0) + jnp.exp(jnp.minimum(u, 0.0))


def silu(u):
    return 0.5 * u * (1.0 + jnp.tanh(0.5 * u))


def dot(a, b):
    return jnp.dot(a, b, preferred_element_type=F32)


def kernel(
    sizes,
    count_ref,
    rows_ref,
    cols_ref,
    used_ref,
    feat_ref,
    blocks_ref,
    wq_ref,
    wk_ref,
    wv_ref,
    wm_ref,
    wo_ref,
    gain_ref,
    out_ref,
    hid,
    halo_0,
    halo_1,
    wide,
    picked,
    send,
    query,
    local,
    res,
    blk,
    summ,
    half,
    quarter,
    piece,
    r1,
    r2,
    r3,
    r4,
    total,
    near_ref,
    far_ref,
    feat_sem,
    blk_sem,
    halo_send,
    halo_recv,
    ar_send,
    ar_recv,
):
    layers, vertices, width, tile, slots, halo_rows = sizes
    halos = (halo_0, halo_1)
    tiles = vertices // tile
    side_tiles = halo_rows // tile
    lanes = width // 2
    steps = vertices // ROWS

    dom, grp = lax.axis_index("dom"), lax.axis_index("grp")
    part = dom * 2 + grp
    parts = NX * NY * NZ * 2
    core = lax.rem(dom, 2)
    y = lax.rem(dom // 2, NY)
    x = lax.rem(dom // (2 * NY), NX)
    z = dom // (2 * NY * NX) * 2 + grp

    def place(x_at, y_at, z_at, core_at):
        return {
            "dom": ((z_at // 2 * NX + x_at) * NY + y_at) * 2 + core_at,
            "grp": lax.rem(z_at, 2),
        }

    def place_of(part_at):
        return {"dom": part_at // 2, "grp": lax.rem(part_at, 2)}

    upper = place_of(lax.rem(part + 1, parts))
    lower = place_of(lax.rem(part + parts - 1, parts))
    twin = place(x, y, z, 1 - core)
    x_others = [place(lax.rem(x + k, NX), y, z, core) for k in range(1, NX)]
    y_others = [place(x, lax.rem(y + k, NY), z, core) for k in range(1, NY)]
    z_others = [place(x, y, lax.rem(z + k, NZ), core) for k in range(1, NZ)]

    some_tiles = ROWS // tile

    def hidden(i):
        return hid[pl.ds(i * some_tiles, some_tiles)].reshape(ROWS, width)

    def set_hidden(i, new):
        hid[pl.ds(i * some_tiles, some_tiles)] = new.reshape(some_tiles, tile, width)

    entry_tiles = ENTRY_ROWS // tile
    entries = vertices // ENTRY_ROWS

    def feat_copy(i):
        at = pl.ds(i * entry_tiles, entry_tiles)
        return pltpu.make_async_copy(feat_ref.at[at], hid.at[at], feat_sem.at[i])

    def blk_copy(i):
        at = pl.ds(i * (tiles // BLOCK_COPIES), tiles // BLOCK_COPIES)
        return pltpu.make_async_copy(blocks_ref.at[at], blk.at[at], blk_sem.at[i])

    for i in range(entries):
        feat_copy(i).start()

    barrier = pltpu.get_barrier_semaphore()
    partners = [upper, lower, twin] + x_others + y_others + z_others
    for partner in partners:
        pl.semaphore_signal(barrier, inc=1, device_id=partner, device_id_type=MESH)

    count = count_ref[0]
    hid[tiles] = jnp.zeros((tile, width), BF16)
    for halo in halos:
        halo[2 * side_tiles] = jnp.zeros((tile, width), BF16)

    def keep(first, new):
        at = first + lax.broadcasted_iota(jnp.int32, (new.shape[0], lanes), 0)
        used = at < count
        return jnp.concatenate(
            [jnp.where(used, new[:, :lanes], 0.0), jnp.where(used, new[:, lanes:], 0.0)], axis=1
        )

    def widen(first, new):
        wide[pl.ds(2 * first, new.shape[0], stride=2), :] = new[:, :lanes]
        wide[pl.ds(2 * first + 1, new.shape[0], stride=2), :] = new[:, lanes:]

    def enter(i):
        feat_copy(i).wait()
        at = pl.ds(i * entry_tiles, entry_tiles)
        kept = keep(i * ENTRY_ROWS, hid[at].reshape(ENTRY_ROWS, width).astype(F32))
        hid[at] = kept.astype(BF16).reshape(entry_tiles, tile, width)
        widen(i * ENTRY_ROWS, kept)

    repeat(0, entries, enter)
    for i in range(BLOCK_COPIES):
        blk_copy(i).start()
    pl.semaphore_wait(barrier, len(partners))

    def halo_copy(layer, side, k):
        at = (1 - side) * side_tiles
        return pltpu.make_async_remote_copy(
            src_ref=send.at[side, k],
            dst_ref=halos[layer].at[at + k],
            send_sem=halo_send.at[side, k],
            recv_sem=halo_recv.at[layer, side, k],
            device_id=lower if side == 0 else upper,
            device_id_type=MESH,
        )

    def gather(layer, first, last):
        def chunk(k):
            for side in range(2):
                base = (2 * k + side) * tile

                def some(i):
                    at = i * UNROLL
                    some_rows = [rows_ref[base + at + u] for u in range(UNROLL)]
                    loaded = [wide[pl.ds(2 * row, 2), :] for row in some_rows]
                    for u in range(UNROLL):
                        picked[side, pl.ds(2 * (at + u), 2), :] = loaded[u]

                repeat(0, tile // UNROLL, some)
                send[side, k, :, :lanes] = picked[side, pl.ds(0, tile, stride=2), :].astype(BF16)
                send[side, k, :, lanes:] = picked[side, pl.ds(1, tile, stride=2), :].astype(BF16)
            for side in range(2):
                halo_copy(layer, side, k).start()

        repeat(first, last, chunk)

    def between(value, low, high):
        return jnp.minimum(jnp.maximum(value, low), high)

    first = tiles + side_tiles * between(1 - part, 0, 1)
    last = tiles + side_tiles * (1 + between(parts - 1 - part, 0, 1))

    def index(t):
        for j in range(slots):
            col = cols_ref[j, t]
            live = between(used_ref[t] - j, 0, 1)
            own = live * between(tiles - col, 0, 1)
            near_ref[t * slots + j] = tiles + (col - tiles) * own
            side = live * between(col - first + 1, 0, 1) * between(last - col, 0, 1)
            far_ref[t * slots + j] = 2 * side_tiles + (col - tiles - 2 * side_tiles) * side

    def exchange(layer, number, src, dst, target):
        return pltpu.make_async_remote_copy(
            src_ref=src,
            dst_ref=dst,
            send_sem=ar_send.at[layer, number],
            recv_sem=ar_recv.at[layer, number],
            device_id=target,
            device_id_type=MESH,
        )

    def start(copies):
        for copy in copies:
            copy.start()

    def wait(copies):
        for copy in copies:
            copy.wait()

    def blocks_of(t):
        return jnp.concatenate([blk[t, j] for j in range(slots)], axis=1)

    for layer in range(layers):
        wk_t = wk_ref[layer].T
        wv, wq = wv_ref[layer], wq_ref[layer]

        gather(layer, 0, FIRST)

        if layer == 0:
            repeat(0, tiles, index)
        summ[...] = jnp.zeros_like(summ)

        def add_summary(i):
            h = hidden(i)
            keys = lax.dot_general(wk_t, h, (((1,), (1,)), ((), ())), preferred_element_type=F32)
            keys = feature_map(keys).astype(BF16)
            values = dot(h, wv).astype(BF16)
            summ[...] += dot(keys, values)

        repeat(0, steps, add_summary)

        def ask(i):
            rows = pl.ds(i * ROWS, ROWS)
            query[rows, :] = feature_map(dot(hidden(i), wq)).astype(BF16)


        def gather_local(i):
            for u in range(GROUP):
                t = i * GROUP + u
                tiles_here = [hid[near_ref[t * slots + j]] for j in range(slots)]
                local[pl.ds(t * tile, tile), :] = dot(
                    blocks_of(t), jnp.concatenate(tiles_here, axis=0)
                )

        loops = tiles // GROUP
        if layer == 0:
            for i in range(BLOCK_COPIES):
                blk_copy(i).wait()

        share = width // 2
        hop = [
            exchange(layer, 0, summ.at[pl.ds((1 - core) * share, share)], r1.at[layer], twin)
        ]
        start(hop)
        repeat(0, steps // 2, ask)
        wait(hop)
        half[...] = summ[pl.ds(core * share, share), :] + r1[layer]

        share //= NX
        hop = [
            exchange(
                layer,
                k,
                half.at[pl.ds(lax.rem(x + k, NX) * share, share)],
                r2.at[layer, k - 1],
                x_others[k - 1],
            )
            for k in range(1, NX)
        ]
        start(hop)
        repeat(steps // 2, steps, ask)
        wait(hop)
        quarter[...] = half[pl.ds(x * share, share), :] + (
            r2[layer, 0] + r2[layer, 1] + r2[layer, 2]
        )

        share //= NY
        hop = [
            exchange(
                layer,
                k + 3,
                quarter.at[pl.ds(lax.rem(y + k, NY) * share, share)],
                r3.at[layer, k - 1],
                y_others[k - 1],
            )
            for k in range(1, NY)
        ]
        start(hop)
        repeat(0, loops // 4, gather_local)
        wait(hop)
        piece[...] = quarter[pl.ds(y * share, share), :] + (
            r3[layer, 0] + r3[layer, 1] + r3[layer, 2]
        )

        hop = [
            exchange(layer, k + 6, piece, r4.at[layer, k - 1], z_others[k - 1])
            for k in range(1, NZ)
        ]
        start(hop)
        gather(layer, FIRST, side_tiles)
        repeat(loops // 4, loops // 2, gather_local)
        wait(hop)
        at = core * (width // 2) + x * (width // 8) + y * share
        total[layer, pl.ds(at, share), :] = piece[...] + (
            r4[layer, 0] + r4[layer, 1] + r4[layer, 2]
        )

        here = total.at[layer, pl.ds(at, share)]
        hop = [
            exchange(layer, k + 9, here, here, y_others[k - 1]) for k in range(1, NY)
        ]
        start(hop)
        repeat(loops // 2, loops // 4 * 3, gather_local)
        wait(hop)
        here = total.at[layer, pl.ds(core * (width // 2) + x * (width // 8), width // 8)]
        hop = [
            exchange(layer, k + 12, here, here, x_others[k - 1]) for k in range(1, NX)
        ]
        start(hop)
        repeat(loops // 4 * 3, loops, gather_local)
        wait(hop)
        here = total.at[layer, pl.ds(core * (width // 2), width // 2)]
        hop = [exchange(layer, 16, here, here, twin)]
        start(hop)
        wait(hop)
        summary = total[layer].astype(BF16)
        wo, wm = wo_ref[layer], wm_ref[layer]
        gain = gain_ref[pl.ds(layer, 1), :]

        def attend(i):
            rows = pl.ds(i * ROWS, ROWS)
            mixed = dot(query[rows, :], summary)
            scale = lax.rsqrt(jnp.mean(mixed * mixed, axis=-1, keepdims=True) + epsilon)
            attended = (mixed * scale * gain).astype(BF16)
            res[rows, :] = hidden(i).astype(F32) + dot(attended, wo)

        repeat(0, steps, attend)

        def arrived(k):
            for side in range(2):
                halo_copy(layer, side, k).wait()

        repeat(0, side_tiles, arrived)

        def finish(i):
            parts_here = []
            for u in range(some_tiles):
                t = i * some_tiles + u
                tiles_here = [halos[layer][far_ref[t * slots + j]] for j in range(slots)]
                both = local[pl.ds(t * tile, tile), :] + dot(
                    blocks_of(t), jnp.concatenate(tiles_here, axis=0)
                )
                parts_here.append(both.astype(BF16))
            message = silu(dot(jnp.concatenate(parts_here, axis=0), wm))
            new = keep(i * ROWS, res[pl.ds(i * ROWS, ROWS), :] + message).astype(BF16)
            if layer < layers - 1:
                set_hidden(i, new)
                widen(i * ROWS, new.astype(F32))
            else:
                out_ref[pl.ds(i * some_tiles, some_tiles)] = new.reshape(some_tiles, tile, width)

        repeat(0, steps, finish)


def on_device(
    node_features,
    vertex_count,
    send_rows,
    block_values,
    block_cols,
    block_count,
    w_query,
    w_key,
    w_value,
    w_message,
    w_out,
    attn_gain,
):
    vertices, width = node_features.shape
    tiles, slots, tile, _ = block_values.shape
    layers = w_query.shape[0]
    halo_rows = send_rows.shape[2]
    side_tiles = halo_rows // tile
    smem = pl.BlockSpec(memory_space=pltpu.SMEM)
    vmem = pl.BlockSpec(memory_space=pltpu.VMEM)
    anywhere = pl.BlockSpec(memory_space=pl.ANY)
    hops = 17

    out = pl.pallas_call(
        functools.partial(kernel, (layers, vertices, width, tile, slots, halo_rows)),
        out_shape=pltpu.VMEM((tiles, tile, width), BF16),
        in_specs=[smem] * 4 + [anywhere] * 2 + [vmem] * 6,
        out_specs=vmem,
        scratch_shapes=[
            pltpu.VMEM((tiles + 1, tile, width), BF16),
            pltpu.VMEM((2 * side_tiles + 1, tile, width), BF16),
            pltpu.VMEM((2 * side_tiles + 1, tile, width), BF16),
            pltpu.VMEM((2 * vertices, width // 2), F32),
            pltpu.VMEM((2, 2 * tile, width // 2), F32),
            pltpu.VMEM((2, side_tiles, tile, width), BF16),
            pltpu.VMEM((vertices, width), BF16),
            pltpu.VMEM((vertices, width), F32),
            pltpu.VMEM((vertices, width), F32),
            pltpu.VMEM((tiles, slots, tile, tile), BF16),
            pltpu.VMEM((width, width), F32),
            pltpu.VMEM((width // 2, width), F32),
            pltpu.VMEM((width // 8, width), F32),
            pltpu.VMEM((width // 32, width), F32),
            pltpu.VMEM((layers, width // 2, width), F32),
            pltpu.VMEM((layers, 3, width // 8, width), F32),
            pltpu.VMEM((layers, 3, width // 32, width), F32),
            pltpu.VMEM((layers, 3, width // 32, width), F32),
            pltpu.VMEM((layers, width, width), F32),
            pltpu.SMEM((tiles * slots,), jnp.int32),
            pltpu.SMEM((tiles * slots,), jnp.int32),
            pltpu.SemaphoreType.DMA((vertices // ENTRY_ROWS,)),
            pltpu.SemaphoreType.DMA((BLOCK_COPIES,)),
            pltpu.SemaphoreType.DMA((2, side_tiles)),
            pltpu.SemaphoreType.DMA((layers, 2, side_tiles)),
            pltpu.SemaphoreType.DMA((layers, hops)),
            pltpu.SemaphoreType.DMA((layers, hops)),
        ],
        compiler_params=pltpu.CompilerParams(
            collective_id=0, has_side_effects=True, vmem_limit_bytes=58 * 2**20
        ),
        name="graph_layers",
    )(
        vertex_count,
        send_rows[0].reshape(2, side_tiles, tile).transpose(1, 0, 2).reshape(-1),
        block_cols.T,
        block_count,
        node_features.reshape(tiles, tile, width),
        block_values,
        w_query,
        w_key,
        w_value,
        w_message,
        w_out,
        attn_gain,
    )
    return out.reshape(vertices, width)


def solution(mesh):
    placed = (
        P(("dom", "grp"), None),
        P(("dom", "grp")),
        P(("dom", "grp"), None, None),
        P(("dom", "grp"), None, None, None),
        P(("dom", "grp"), None),
        P(("dom", "grp")),
        P(),
        P(),
        P(),
        P(),
        P(),
        P(),
    )
    return jax.shard_map(
        on_device, mesh=mesh, in_specs=placed, out_specs=P(("dom", "grp"), None), check_vma=False
    )
```

```python
import functools

import jax
import jax.numpy as jnp
from jax import lax
from jax.experimental import pallas as pl
from jax.experimental.pallas import tpu as pltpu
from jax.sharding import PartitionSpec as P

MESH = pl.DeviceIdType.MESH
epsilon = 1e-06
F32 = jnp.float32
BF16 = jnp.bfloat16

NX, NY, NZ = 4, 4, 4
ROWS = 4096
ENTRY_ROWS = 1024
FINISH = 512
GROUP = 16
UNROLL = 32
BLOCK_COPIES = 4
CHUNK = 2
FIRST = 1
SECOND = 3


def repeat(start, stop, body):
    def step(i, carry):
        body(i)
        return carry

    lax.fori_loop(start, stop, step, 0)


def feature_map(u):
    return jnp.maximum(u, 0.0) + jnp.exp(jnp.minimum(u, 0.0))


def silu(u):
    h = 0.5 * u
    return h + h * jnp.tanh(h)


def dot(a, b):
    return jnp.dot(a, b, preferred_element_type=F32)


def kernel(
    sizes,
    count_ref,
    rows_ref,
    cols_ref,
    used_ref,
    feat_ref,
    blocks_ref,
    wq_hbm,
    wk_hbm,
    wv_hbm,
    wm_hbm,
    wo_hbm,
    gain_hbm,
    out_ref,
    wq_ref,
    wk_ref,
    wv_ref,
    wm_ref,
    wo_ref,
    gain_ref,
    hid,
    halo_0,
    halo_1,
    wide,
    picked,
    send,
    query,
    local,
    res,
    blk,
    summ,
    half,
    quarter,
    piece,
    r1,
    r2,
    r3,
    r4,
    total,
    near_ref,
    far_ref,
    weight_sem,
    feat_sem,
    blk_sem,
    halo_send,
    halo_recv,
    ar_send,
    ar_recv,
):
    layers, vertices, width, tile, slots, halo_rows = sizes
    halos = (halo_0, halo_1)
    tiles = vertices // tile
    side_tiles = halo_rows // tile
    lanes = width // 2
    steps = vertices // ROWS

    dom, grp = lax.axis_index("dom"), lax.axis_index("grp")
    part = dom * 2 + grp
    parts = NX * NY * NZ * 2
    core = lax.rem(dom, 2)
    y = lax.rem(dom // 2, NY)
    x = lax.rem(dom // (2 * NY), NX)
    z = dom // (2 * NY * NX) * 2 + grp

    def place(x_at, y_at, z_at, core_at):
        return {
            "dom": ((z_at // 2 * NX + x_at) * NY + y_at) * 2 + core_at,
            "grp": lax.rem(z_at, 2),
        }

    def place_of(part_at):
        return {"dom": part_at // 2, "grp": lax.rem(part_at, 2)}

    upper = place_of(lax.rem(part + 1, parts))
    lower = place_of(lax.rem(part + parts - 1, parts))
    twin = place(x, y, z, 1 - core)
    x_others = [place(lax.rem(x + k, NX), y, z, core) for k in range(1, NX)]
    y_others = [place(x, lax.rem(y + k, NY), z, core) for k in range(1, NY)]
    z_others = [place(x, y, lax.rem(z + k, NZ), core) for k in range(1, NZ)]

    some_tiles = ROWS // tile

    def hidden(i):
        return hid[pl.ds(i * some_tiles, some_tiles)].reshape(ROWS, width)

    def set_hidden(i, new):
        hid[pl.ds(i * some_tiles, some_tiles)] = new.reshape(some_tiles, tile, width)

    entry_tiles = ENTRY_ROWS // tile
    entries = vertices // ENTRY_ROWS

    def feat_copy(i):
        at = pl.ds(i * entry_tiles, entry_tiles)
        return pltpu.make_async_copy(feat_ref.at[at], hid.at[at], feat_sem.at[i])

    def blk_copy(i):
        at = pl.ds(i * (tiles // BLOCK_COPIES), tiles // BLOCK_COPIES)
        return pltpu.make_async_copy(blocks_ref.at[at], blk.at[at], blk_sem.at[i])

    weight_copies = [
        pltpu.make_async_copy(src, dst, weight_sem.at[i])
        for i, (src, dst) in enumerate(
            (
                (wk_hbm, wk_ref),
                (wv_hbm, wv_ref),
                (wq_hbm, wq_ref),
                (wm_hbm, wm_ref),
                (wo_hbm, wo_ref),
                (gain_hbm, gain_ref),
            )
        )
    ]
    for i in range(entries):
        feat_copy(i).start()
    for copy in weight_copies:
        copy.start()

    barrier = pltpu.get_barrier_semaphore()
    partners = [upper, lower, twin] + x_others + y_others + z_others
    for partner in partners:
        pl.semaphore_signal(barrier, inc=1, device_id=partner, device_id_type=MESH)

    count = count_ref[0]
    hid[tiles] = jnp.zeros((tile, width), BF16)
    for halo in halos:
        halo[2 * side_tiles] = jnp.zeros((tile, width), BF16)

    def keep(first, new):
        at = first + lax.broadcasted_iota(jnp.int32, (new.shape[0], lanes), 0)
        used = at < count
        return jnp.concatenate(
            [jnp.where(used, new[:, :lanes], 0.0), jnp.where(used, new[:, lanes:], 0.0)], axis=1
        )

    def widen(first, new):
        wide[pl.ds(2 * first, new.shape[0], stride=2), :] = new[:, :lanes]
        wide[pl.ds(2 * first + 1, new.shape[0], stride=2), :] = new[:, lanes:]

    def enter(i):
        feat_copy(i).wait()
        at = pl.ds(i * entry_tiles, entry_tiles)
        kept = keep(i * ENTRY_ROWS, hid[at].reshape(ENTRY_ROWS, width).astype(F32))
        hid[at] = kept.astype(BF16).reshape(entry_tiles, tile, width)
        widen(i * ENTRY_ROWS, kept)

    repeat(0, entries, enter)
    for i in range(BLOCK_COPIES):
        blk_copy(i).start()
    pl.semaphore_wait(barrier, len(partners))

    def halo_copy(layer, side, k):
        at = (1 - side) * side_tiles
        return pltpu.make_async_remote_copy(
            src_ref=send.at[side, pl.ds(k * CHUNK, CHUNK)],
            dst_ref=halos[layer].at[pl.ds(at + k * CHUNK, CHUNK)],
            send_sem=halo_send.at[side, k],
            recv_sem=halo_recv.at[layer, side, k],
            device_id=lower if side == 0 else upper,
            device_id_type=MESH,
        )

    def gather(layer, first, last):
        def one_tile(side, k):
            base = (2 * k + side) * tile

            def some(i):
                at = i * UNROLL
                some_rows = [rows_ref[base + at + u] for u in range(UNROLL)]
                loaded = [wide[pl.ds(2 * row, 2), :] for row in some_rows]
                for u in range(UNROLL):
                    picked[side, pl.ds(2 * (at + u), 2), :] = loaded[u]

            repeat(0, tile // UNROLL, some)
            send[side, k, :, :lanes] = picked[side, pl.ds(0, tile, stride=2), :].astype(BF16)
            send[side, k, :, lanes:] = picked[side, pl.ds(1, tile, stride=2), :].astype(BF16)

        def chunk(k):
            for side in range(2):
                if CHUNK == 1:
                    one_tile(side, k)
                else:
                    repeat(k * CHUNK, (k + 1) * CHUNK, lambda t: one_tile(side, t))
            for side in range(2):
                halo_copy(layer, side, k).start()

        repeat(first, last, chunk)

    def between(value, low, high):
        return jnp.minimum(jnp.maximum(value, low), high)

    first = tiles + side_tiles * between(1 - part, 0, 1)
    last = tiles + side_tiles * (1 + between(parts - 1 - part, 0, 1))

    def index(t):
        for j in range(slots):
            col = cols_ref[j, t]
            live = between(used_ref[t] - j, 0, 1)
            own = live * between(tiles - col, 0, 1)
            near_ref[t * slots + j] = tiles + (col - tiles) * own
            side = live * between(col - first + 1, 0, 1) * between(last - col, 0, 1)
            far_ref[t * slots + j] = 2 * side_tiles + (col - tiles - 2 * side_tiles) * side

    def exchange(layer, number, src, dst, target):
        return pltpu.make_async_remote_copy(
            src_ref=src,
            dst_ref=dst,
            send_sem=ar_send.at[layer, number],
            recv_sem=ar_recv.at[layer, number],
            device_id=target,
            device_id_type=MESH,
        )

    def start(copies):
        for copy in copies:
            copy.start()

    def wait(copies):
        for copy in copies:
            copy.wait()

    def blocks_of(t):
        return jnp.concatenate([blk[t, j] for j in range(slots)], axis=1)

    for layer in range(layers):
        gather(layer, 0, FIRST)
        if layer == 0:
            for copy in weight_copies:
                copy.wait()
        wk_t = wk_ref[layer].T
        wv, wq = wv_ref[layer], wq_ref[layer]
        summ[...] = jnp.zeros_like(summ)

        def add_summary(i):
            h = hidden(i)
            keys = lax.dot_general(wk_t, h, (((1,), (1,)), ((), ())), preferred_element_type=F32)
            keys = feature_map(keys).astype(BF16)
            values = dot(h, wv).astype(BF16)
            summ[...] += dot(keys, values)

        repeat(0, steps, add_summary)

        def ask(i):
            rows = pl.ds(i * ROWS, ROWS)
            query[rows, :] = feature_map(dot(hidden(i), wq)).astype(BF16)


        def gather_local(i):
            for u in range(GROUP):
                t = i * GROUP + u
                tiles_here = [hid[near_ref[t * slots + j]] for j in range(slots)]
                local[pl.ds(t * tile, tile), :] = dot(
                    blocks_of(t), jnp.concatenate(tiles_here, axis=0)
                )

        loops = tiles // GROUP

        gather(layer, FIRST, SECOND)

        share = width // 2
        hop = [
            exchange(layer, 0, summ.at[pl.ds((1 - core) * share, share)], r1.at[layer], twin)
        ]
        start(hop)
        if layer == 0:
            repeat(0, tiles, index)
        else:
            repeat(0, steps // 2, ask)
        wait(hop)
        half[...] = summ[pl.ds(core * share, share), :] + r1[layer]

        share //= NX
        hop = [
            exchange(
                layer,
                k,
                half.at[pl.ds(lax.rem(x + k, NX) * share, share)],
                r2.at[layer, k - 1],
                x_others[k - 1],
            )
            for k in range(1, NX)
        ]
        start(hop)
        repeat(0 if layer == 0 else steps // 2, steps, ask)
        wait(hop)
        quarter[...] = half[pl.ds(x * share, share), :] + (
            r2[layer, 0] + r2[layer, 1] + r2[layer, 2]
        )

        hop = [
            exchange(layer, k + 3, quarter, r3.at[layer, k - 1], y_others[k - 1])
            for k in range(1, NY)
        ]
        start(hop)
        if layer == 0:
            for i in range(BLOCK_COPIES):
                blk_copy(i).wait()
        repeat(0, loops // 4, gather_local)
        wait(hop)
        piece[...] = quarter[...] + (r3[layer, 0] + r3[layer, 1] + r3[layer, 2])

        hop = [
            exchange(layer, k + 6, piece, r4.at[layer, k - 1], z_others[k - 1])
            for k in range(1, NZ)
        ]
        start(hop)
        gather(layer, SECOND, side_tiles // CHUNK)
        repeat(loops // 4, loops // 2, gather_local)
        wait(hop)
        at = core * (width // 2) + x * share
        total[layer, pl.ds(at, share), :] = piece[...] + (
            r4[layer, 0] + r4[layer, 1] + r4[layer, 2]
        )

        here = total.at[layer, pl.ds(at, share)]
        hop = [
            exchange(layer, k + 9, here, here, x_others[k - 1]) for k in range(1, NX)
        ]
        start(hop)
        repeat(loops // 2, loops // 4 * 3, gather_local)
        wait(hop)
        here = total.at[layer, pl.ds(core * (width // 2), width // 2)]
        hop = [exchange(layer, 13, here, here, twin)]
        start(hop)
        repeat(loops // 4 * 3, loops, gather_local)
        wait(hop)
        summary = total[layer].astype(BF16)
        wo, wm = wo_ref[layer], wm_ref[layer]
        gain = gain_ref[pl.ds(layer, 1), :]

        def attend(i):
            rows = pl.ds(i * ROWS, ROWS)
            mixed = dot(query[rows, :], summary)
            scale = lax.rsqrt(jnp.mean(mixed * mixed, axis=-1, keepdims=True) + epsilon)
            attended = (mixed * scale * gain).astype(BF16)
            res[rows, :] = hidden(i).astype(F32) + dot(attended, wo)

        repeat(0, steps, attend)

        def arrived(k):
            for side in range(2):
                halo_copy(layer, side, k).wait()

        repeat(0, side_tiles // CHUNK, arrived)

        def finish_some(first):
            parts_here = []
            for u in range(FINISH // tile):
                t = first * (FINISH // tile) + u
                tiles_here = [halos[layer][far_ref[t * slots + j]] for j in range(slots)]
                both = local[pl.ds(t * tile, tile), :] + dot(
                    blocks_of(t), jnp.concatenate(tiles_here, axis=0)
                )
                parts_here.append(both.astype(BF16))
            message = silu(dot(jnp.concatenate(parts_here, axis=0), wm))
            rows = first * FINISH
            new = keep(rows, res[pl.ds(rows, FINISH), :] + message).astype(BF16)
            at = pl.ds(first * (FINISH // tile), FINISH // tile)
            if layer < layers - 1:
                hid[at] = new.reshape(FINISH // tile, tile, width)
                widen(rows, new.astype(F32))
            else:
                out_ref[at] = new.reshape(FINISH // tile, tile, width)

        def finish(i):
            for k in range(ROWS // FINISH):
                finish_some(i * (ROWS // FINISH) + k)

        repeat(0, steps, finish)


def on_device(
    node_features,
    vertex_count,
    send_rows,
    block_values,
    block_cols,
    block_count,
    w_query,
    w_key,
    w_value,
    w_message,
    w_out,
    attn_gain,
):
    vertices, width = node_features.shape
    tiles, slots, tile, _ = block_values.shape
    layers = w_query.shape[0]
    halo_rows = send_rows.shape[2]
    side_tiles = halo_rows // tile
    smem = pl.BlockSpec(memory_space=pltpu.SMEM)
    vmem = pl.BlockSpec(memory_space=pltpu.VMEM)
    anywhere = pl.BlockSpec(memory_space=pl.ANY)
    hops = 14

    out = pl.pallas_call(
        functools.partial(kernel, (layers, vertices, width, tile, slots, halo_rows)),
        out_shape=pltpu.VMEM((tiles, tile, width), BF16),
        in_specs=[smem] * 4 + [anywhere] * 8,
        out_specs=vmem,
        scratch_shapes=[pltpu.VMEM((layers, width, width), BF16)] * 5
        + [
            pltpu.VMEM((layers, width), F32),
            pltpu.VMEM((tiles + 1, tile, width), BF16),
            pltpu.VMEM((2 * side_tiles + 1, tile, width), BF16),
            pltpu.VMEM((2 * side_tiles + 1, tile, width), BF16),
            pltpu.VMEM((2 * vertices, width // 2), F32),
            pltpu.VMEM((2, 2 * tile, width // 2), F32),
            pltpu.VMEM((2, side_tiles, tile, width), BF16),
            pltpu.VMEM((vertices, width), BF16),
            pltpu.VMEM((vertices, width), F32),
            pltpu.VMEM((vertices, width), F32),
            pltpu.VMEM((tiles, slots, tile, tile), BF16),
            pltpu.VMEM((width, width), F32),
            pltpu.VMEM((width // 2, width), F32),
            pltpu.VMEM((width // 8, width), F32),
            pltpu.VMEM((width // 8, width), F32),
            pltpu.VMEM((layers, width // 2, width), F32),
            pltpu.VMEM((layers, 3, width // 8, width), F32),
            pltpu.VMEM((layers, 3, width // 8, width), F32),
            pltpu.VMEM((layers, 3, width // 8, width), F32),
            pltpu.VMEM((layers, width, width), F32),
            pltpu.SMEM((tiles * slots,), jnp.int32),
            pltpu.SMEM((tiles * slots,), jnp.int32),
            pltpu.SemaphoreType.DMA((6,)),
            pltpu.SemaphoreType.DMA((vertices // ENTRY_ROWS,)),
            pltpu.SemaphoreType.DMA((BLOCK_COPIES,)),
            pltpu.SemaphoreType.DMA((2, side_tiles // CHUNK)),
            pltpu.SemaphoreType.DMA((layers, 2, side_tiles // CHUNK)),
            pltpu.SemaphoreType.DMA((layers, hops)),
            pltpu.SemaphoreType.DMA((layers, hops)),
        ],
        compiler_params=pltpu.CompilerParams(
            collective_id=0, has_side_effects=True, vmem_limit_bytes=58 * 2**20
        ),
        name="graph_layers",
    )(
        vertex_count,
        send_rows[0].reshape(2, side_tiles, tile).transpose(1, 0, 2).reshape(-1),
        block_cols.T,
        block_count,
        node_features.reshape(tiles, tile, width),
        block_values,
        w_query,
        w_key,
        w_value,
        w_message,
        w_out,
        attn_gain,
    )
    return out.reshape(vertices, width)


def solution(mesh):
    placed = (
        P(("dom", "grp"), None),
        P(("dom", "grp")),
        P(("dom", "grp"), None, None),
        P(("dom", "grp"), None, None, None),
        P(("dom", "grp"), None),
        P(("dom", "grp")),
        P(),
        P(),
        P(),
        P(),
        P(),
        P(),
    )
    return jax.shard_map(
        on_device, mesh=mesh, in_specs=placed, out_specs=P(("dom", "grp"), None), check_vma=False
    )
```

```python
import functools

import jax
import jax.numpy as jnp
from jax import lax
from jax.experimental import pallas as pl
from jax.experimental.pallas import tpu as pltpu
from jax.sharding import PartitionSpec as P

MESH = pl.DeviceIdType.MESH
epsilon = 1e-06
F32 = jnp.float32
BF16 = jnp.bfloat16

NX, NY, NZ = 4, 4, 4
ROWS = 4096
ENTRY_ROWS = 1024
FINISH = 1024
GROUP = 16
UNROLL = 32
BLOCK_COPIES = 4
CHUNKS = (1, 1, 2, 2, 2, 4, 4)
FIRST = 2
SECOND = 4
THIRD = 5


def repeat(start, stop, body):
    def step(i, carry):
        body(i)
        return carry

    lax.fori_loop(start, stop, step, 0)


def feature_map(u):
    return jnp.maximum(u, 0.0) + jnp.exp(jnp.minimum(u, 0.0))


def silu_of_twice(h):
    return h + h * jnp.tanh(h)


def dot(a, b):
    return jnp.dot(a, b, preferred_element_type=F32)


def kernel(
    sizes,
    count_hbm,
    rows_hbm,
    cols_hbm,
    used_hbm,
    feat_ref,
    blocks_ref,
    wq_hbm,
    wk_hbm,
    wv_hbm,
    wm_hbm,
    wo_hbm,
    gain_hbm,
    out_ref,
    wq_ref,
    wk_ref,
    wv_ref,
    wm_ref,
    wo_ref,
    gain_ref,
    hid,
    lifted,
    halo_0,
    halo_1,
    wide,
    picked,
    send,
    query,
    local,
    res,
    blk,
    summ,
    half,
    quarter,
    piece,
    r1,
    r2,
    r3,
    r4,
    r5,
    coarse,
    total,
    count_ref,
    rows_ref,
    cols_ref,
    used_ref,
    near_ref,
    far_ref,
    small_sem,
    weight_sem,
    feat_sem,
    blk_sem,
    halo_send,
    halo_recv,
    ar_send,
    ar_recv,
):
    layers, vertices, width, tile, slots, halo_rows = sizes
    halos = (halo_0, halo_1)
    tiles = vertices // tile
    side_tiles = halo_rows // tile
    lanes = width // 2
    steps = vertices // ROWS

    dom, grp = lax.axis_index("dom"), lax.axis_index("grp")
    part = dom * 2 + grp
    parts = NX * NY * NZ * 2
    core = lax.rem(dom, 2)
    y = lax.rem(dom // 2, NY)
    x = lax.rem(dom // (2 * NY), NX)
    z = dom // (2 * NY * NX) * 2 + grp

    def place(x_at, y_at, z_at, core_at):
        return {
            "dom": ((z_at // 2 * NX + x_at) * NY + y_at) * 2 + core_at,
            "grp": lax.rem(z_at, 2),
        }

    def place_of(part_at):
        return {"dom": part_at // 2, "grp": lax.rem(part_at, 2)}

    upper = place_of(lax.rem(part + 1, parts))
    lower = place_of(lax.rem(part + parts - 1, parts))
    twin = place(x, y, z, 1 - core)
    x_others = [place(lax.rem(x + k, NX), y, z, core) for k in range(1, NX)]
    y_others = [place(x, lax.rem(y + k, NY), z, core) for k in range(1, NY)]
    z_far = place(x, y, NZ - 1 - z, core)
    z_near = {"dom": dom, "grp": 1 - grp}

    some_tiles = ROWS // tile

    def hidden(i):
        return hid[pl.ds(i * some_tiles, some_tiles)].reshape(ROWS, width)

    def set_hidden(i, new):
        hid[pl.ds(i * some_tiles, some_tiles)] = new.reshape(some_tiles, tile, width)

    entry_tiles = ENTRY_ROWS // tile
    entries = vertices // ENTRY_ROWS

    def feat_copy(i):
        at = pl.ds(i * entry_tiles, entry_tiles)
        return pltpu.make_async_copy(feat_ref.at[at], hid.at[at], feat_sem.at[i])

    def blk_copy(i):
        at = pl.ds(i * (tiles // BLOCK_COPIES), tiles // BLOCK_COPIES)
        return pltpu.make_async_copy(blocks_ref.at[at], blk.at[at], blk_sem.at[i])

    weight_copies = [
        pltpu.make_async_copy(src, dst, weight_sem.at[i])
        for i, (src, dst) in enumerate(
            (
                (wk_hbm, wk_ref),
                (wv_hbm, wv_ref),
                (wq_hbm, wq_ref),
                (wm_hbm, wm_ref),
                (wo_hbm, wo_ref),
                (gain_hbm, gain_ref),
            )
        )
    ]
    for i in range(entries):
        feat_copy(i).start()
    small_copies = [
        pltpu.make_async_copy(src, dst, small_sem.at[i])
        for i, (src, dst) in enumerate(
            (
                (count_hbm, count_ref),
                (rows_hbm, rows_ref),
                (cols_hbm, cols_ref),
                (used_hbm, used_ref),
            )
        )
    ]
    for copy in small_copies + weight_copies:
        copy.start()

    barrier = pltpu.get_barrier_semaphore()
    partners = [upper, lower, twin, z_far, z_near] + x_others + y_others
    for partner in partners:
        pl.semaphore_signal(barrier, inc=1, device_id=partner, device_id_type=MESH)

    small_copies[0].wait()
    count = count_ref[0]
    lifted[tiles] = jnp.zeros((tile, width), BF16)
    for halo in halos:
        halo[2 * side_tiles] = jnp.zeros((tile, width), BF16)

    def keep(first, new):
        at = first + lax.broadcasted_iota(jnp.int32, (new.shape[0], lanes), 0)
        used = at < count
        return jnp.concatenate(
            [jnp.where(used, new[:, :lanes], 0.0), jnp.where(used, new[:, lanes:], 0.0)], axis=1
        )

    def widen(first, new):
        wide[pl.ds(2 * first, new.shape[0], stride=2), :] = new[:, :lanes]
        wide[pl.ds(2 * first + 1, new.shape[0], stride=2), :] = new[:, lanes:]

    def enter(i):
        feat_copy(i).wait()
        at = pl.ds(i * entry_tiles, entry_tiles)
        kept = keep(i * ENTRY_ROWS, hid[at].reshape(ENTRY_ROWS, width).astype(F32))
        hid[at] = kept.astype(BF16).reshape(entry_tiles, tile, width)
        widen(i * ENTRY_ROWS, kept)

    repeat(0, entries, enter)
    for i in range(BLOCK_COPIES):
        blk_copy(i).start()
    for copy in small_copies[1:]:
        copy.wait()
    pl.semaphore_wait(barrier, len(partners))

    def halo_copy(layer, side, k):
        at = (1 - side) * side_tiles + sum(CHUNKS[:k])
        return pltpu.make_async_remote_copy(
            src_ref=send.at[side, pl.ds(sum(CHUNKS[:k]), CHUNKS[k])],
            dst_ref=halos[layer].at[pl.ds(at, CHUNKS[k])],
            send_sem=halo_send.at[side, k],
            recv_sem=halo_recv.at[layer, side, k],
            device_id=lower if side == 0 else upper,
            device_id_type=MESH,
        )

    def gather(layer, first, last):
        def one_tile(k):
            for side in range(2):
                base = (2 * k + side) * tile

                def some(i):
                    at = i * UNROLL
                    some_rows = [rows_ref[base + at + u] for u in range(UNROLL)]
                    loaded = [wide[pl.ds(2 * row, 2), :] for row in some_rows]
                    for u in range(UNROLL):
                        picked[side, pl.ds(2 * (at + u), 2), :] = loaded[u]

                repeat(0, tile // UNROLL, some)
                send[side, k, :, :lanes] = picked[side, pl.ds(0, tile, stride=2), :].astype(BF16)
                send[side, k, :, lanes:] = picked[side, pl.ds(1, tile, stride=2), :].astype(BF16)

        for k in range(first, last):
            repeat(sum(CHUNKS[:k]), sum(CHUNKS[: k + 1]), one_tile)
            for side in range(2):
                halo_copy(layer, side, k).start()

    def between(value, low, high):
        return jnp.minimum(jnp.maximum(value, low), high)

    first = tiles + side_tiles * between(1 - part, 0, 1)
    last = tiles + side_tiles * (1 + between(parts - 1 - part, 0, 1))

    def index(t):
        for j in range(slots):
            col = cols_ref[j, t]
            live = between(used_ref[t] - j, 0, 1)
            own = live * between(tiles - col, 0, 1)
            near_ref[t * slots + j] = tiles + (col - tiles) * own
            side = live * between(col - first + 1, 0, 1) * between(last - col, 0, 1)
            far_ref[t * slots + j] = 2 * side_tiles + (col - tiles - 2 * side_tiles) * side

    def exchange(layer, number, src, dst, target):
        return pltpu.make_async_remote_copy(
            src_ref=src,
            dst_ref=dst,
            send_sem=ar_send.at[layer, number],
            recv_sem=ar_recv.at[layer, number],
            device_id=target,
            device_id_type=MESH,
        )

    def start(copies):
        for copy in copies:
            copy.start()

    def wait(copies):
        for copy in copies:
            copy.wait()

    def blocks_of(t):
        return jnp.concatenate([blk[t, j] for j in range(slots)], axis=1)

    for layer in range(layers):
        gather(layer, 0, FIRST)
        if layer == 0:
            for copy in weight_copies:
                copy.wait()
        wk_t = wk_ref[layer].T
        wv, wq, wo = wv_ref[layer], wq_ref[layer], wo_ref[layer]
        wm = (0.5 * wm_ref[layer].astype(F32)).astype(BF16)
        summ[...] = jnp.zeros_like(summ)

        def add_summary(i):
            h = hidden(i)
            keys = lax.dot_general(wk_t, h, (((1,), (1,)), ((), ())), preferred_element_type=F32)
            keys = feature_map(keys).astype(BF16)
            values = dot(h, wv).astype(BF16)
            summ[...] += dot(keys, values)

        repeat(0, steps, add_summary)

        def ask(i):
            rows = pl.ds(i * ROWS, ROWS)
            h = hidden(i)
            query[rows, :] = feature_map(dot(h, wq)).astype(BF16)
            ahead = dot(h, wm).astype(BF16)
            lifted[pl.ds(i * some_tiles, some_tiles)] = ahead.reshape(some_tiles, tile, width)


        def gather_local(i):
            for u in range(GROUP):
                t = i * GROUP + u
                tiles_here = [lifted[near_ref[t * slots + j]] for j in range(slots)]
                local[pl.ds(t * tile, tile), :] = dot(
                    blocks_of(t), jnp.concatenate(tiles_here, axis=0)
                )

        loops = tiles // GROUP

        gather(layer, FIRST, SECOND)

        share = width // 2
        hop = [
            exchange(layer, 0, summ.at[pl.ds((1 - core) * share, share)], r1.at[layer], twin)
        ]
        start(hop)
        if layer == 0:
            repeat(0, tiles, index)
        else:
            repeat(0, steps // 2, ask)
        wait(hop)
        half[...] = summ[pl.ds(core * share, share), :] + r1[layer]

        share //= NX
        hop = [
            exchange(
                layer,
                k,
                half.at[pl.ds(lax.rem(x + k, NX) * share, share)],
                r2.at[layer, k - 1],
                x_others[k - 1],
            )
            for k in range(1, NX)
        ]
        start(hop)
        repeat(0 if layer == 0 else steps // 2, steps, ask)
        wait(hop)
        quarter[...] = half[pl.ds(x * share, share), :] + (
            r2[layer, 0] + r2[layer, 1] + r2[layer, 2]
        )

        hop = [
            exchange(layer, k + 3, quarter, r3.at[layer, k - 1], y_others[k - 1])
            for k in range(1, NY)
        ]
        start(hop)
        if layer == 0:
            for i in range(BLOCK_COPIES):
                blk_copy(i).wait()
        repeat(0, loops // 4, gather_local)
        wait(hop)
        piece[...] = quarter[...] + (r3[layer, 0] + r3[layer, 1] + r3[layer, 2])

        hop = [exchange(layer, 7, piece, r4.at[layer], z_far)]
        start(hop)
        gather(layer, SECOND, THIRD)
        repeat(loops // 4, loops // 2, gather_local)
        wait(hop)
        coarse[...] = (piece[...] + r4[layer]).astype(BF16)
        hop = [exchange(layer, 8, coarse, r5.at[layer], z_near)]
        start(hop)
        gather(layer, THIRD, len(CHUNKS))
        wait(hop)
        at = core * (width // 2) + x * share
        total[layer, pl.ds(at, share), :] = coarse[...].astype(F32) + r5[layer].astype(F32)

        here = total.at[layer, pl.ds(at, share)]
        hop = [
            exchange(layer, k + 9, here, here, x_others[k - 1]) for k in range(1, NX)
        ]
        start(hop)
        repeat(loops // 2, loops // 4 * 3, gather_local)
        wait(hop)
        here = total.at[layer, pl.ds(core * (width // 2), width // 2)]
        hop = [exchange(layer, 13, here, here, twin)]
        start(hop)
        repeat(loops // 4 * 3, loops, gather_local)
        wait(hop)
        summary = total[layer].astype(BF16)
        gain = gain_ref[pl.ds(layer, 1), :]

        def attend(i):
            rows = pl.ds(i * ROWS, ROWS)
            mixed = dot(query[rows, :], summary)
            scale = lax.rsqrt(jnp.mean(mixed * mixed, axis=-1, keepdims=True) + epsilon)
            attended = (mixed * scale * gain).astype(BF16)
            res[rows, :] = hidden(i).astype(F32) + dot(attended, wo)

        repeat(0, steps, attend)

        for k in range(len(CHUNKS)):
            for side in range(2):
                halo_copy(layer, side, k).wait()
                at = pl.ds((1 - side) * side_tiles + sum(CHUNKS[:k]), CHUNKS[k])
                ahead = dot(halos[layer][at].reshape(CHUNKS[k] * tile, width), wm)
                halos[layer][at] = ahead.astype(BF16).reshape(CHUNKS[k], tile, width)

        def finish_some(first):
            parts_here = []
            for u in range(FINISH // tile):
                t = first * (FINISH // tile) + u
                tiles_here = [halos[layer][far_ref[t * slots + j]] for j in range(slots)]
                parts_here.append(dot(blocks_of(t), jnp.concatenate(tiles_here, axis=0)))
            both = local[pl.ds(first * FINISH, FINISH), :] + jnp.concatenate(parts_here, axis=0)
            message = silu_of_twice(both)
            rows = first * FINISH
            new = keep(rows, res[pl.ds(rows, FINISH), :] + message).astype(BF16)
            at = pl.ds(first * (FINISH // tile), FINISH // tile)
            if layer < layers - 1:
                hid[at] = new.reshape(FINISH // tile, tile, width)
                widen(rows, new.astype(F32))
            else:
                out_ref[at] = new.reshape(FINISH // tile, tile, width)

        def finish(i):
            for k in range(ROWS // FINISH):
                finish_some(i * (ROWS // FINISH) + k)

        repeat(0, steps, finish)


def on_device(
    node_features,
    vertex_count,
    send_rows,
    block_values,
    block_cols,
    block_count,
    w_query,
    w_key,
    w_value,
    w_message,
    w_out,
    attn_gain,
):
    vertices, width = node_features.shape
    tiles, slots, tile, _ = block_values.shape
    layers = w_query.shape[0]
    halo_rows = send_rows.shape[2]
    side_tiles = halo_rows // tile
    vmem = pl.BlockSpec(memory_space=pltpu.VMEM)
    anywhere = pl.BlockSpec(memory_space=pl.ANY)
    hops = 14

    out = pl.pallas_call(
        functools.partial(kernel, (layers, vertices, width, tile, slots, halo_rows)),
        out_shape=pltpu.VMEM((tiles, tile, width), BF16),
        in_specs=[anywhere] * 12,
        out_specs=vmem,
        scratch_shapes=[pltpu.VMEM((layers, width, width), BF16)] * 5
        + [
            pltpu.VMEM((layers, width), F32),
            pltpu.VMEM((tiles, tile, width), BF16),
            pltpu.VMEM((tiles + 1, tile, width), BF16),
            pltpu.VMEM((2 * side_tiles + 1, tile, width), BF16),
            pltpu.VMEM((2 * side_tiles + 1, tile, width), BF16),
            pltpu.VMEM((2 * vertices, width // 2), F32),
            pltpu.VMEM((2, 2 * tile, width // 2), F32),
            pltpu.VMEM((2, side_tiles, tile, width), BF16),
            pltpu.VMEM((vertices, width), BF16),
            pltpu.VMEM((vertices, width), F32),
            pltpu.VMEM((vertices, width), F32),
            pltpu.VMEM((tiles, slots, tile, tile), BF16),
            pltpu.VMEM((width, width), F32),
            pltpu.VMEM((width // 2, width), F32),
            pltpu.VMEM((width // 8, width), F32),
            pltpu.VMEM((width // 8, width), F32),
            pltpu.VMEM((layers, width // 2, width), F32),
            pltpu.VMEM((layers, 3, width // 8, width), F32),
            pltpu.VMEM((layers, 3, width // 8, width), F32),
            pltpu.VMEM((layers, width // 8, width), F32),
            pltpu.VMEM((layers, width // 8, width), BF16),
            pltpu.VMEM((width // 8, width), BF16),
            pltpu.VMEM((layers, width, width), F32),
            pltpu.SMEM((1,), jnp.int32),
            pltpu.SMEM((2 * halo_rows,), jnp.int32),
            pltpu.SMEM((slots, tiles), jnp.int32),
            pltpu.SMEM((tiles,), jnp.int32),
            pltpu.SMEM((tiles * slots,), jnp.int32),
            pltpu.SMEM((tiles * slots,), jnp.int32),
            pltpu.SemaphoreType.DMA((4,)),
            pltpu.SemaphoreType.DMA((6,)),
            pltpu.SemaphoreType.DMA((vertices // ENTRY_ROWS,)),
            pltpu.SemaphoreType.DMA((BLOCK_COPIES,)),
            pltpu.SemaphoreType.DMA((2, len(CHUNKS))),
            pltpu.SemaphoreType.DMA((layers, 2, len(CHUNKS))),
            pltpu.SemaphoreType.DMA((layers, hops)),
            pltpu.SemaphoreType.DMA((layers, hops)),
        ],
        compiler_params=pltpu.CompilerParams(
            collective_id=0, has_side_effects=True, vmem_limit_bytes=59 * 2**20
        ),
        name="graph_layers",
    )(
        vertex_count,
        send_rows[0].reshape(2, side_tiles, tile).transpose(1, 0, 2).reshape(-1),
        block_cols.T,
        block_count,
        node_features.reshape(tiles, tile, width),
        block_values,
        w_query,
        w_key,
        w_value,
        w_message,
        w_out,
        attn_gain,
    )
    return out.reshape(vertices, width)


def solution(mesh):
    placed = (
        P(("dom", "grp"), None),
        P(("dom", "grp")),
        P(("dom", "grp"), None, None),
        P(("dom", "grp"), None, None, None),
        P(("dom", "grp"), None),
        P(("dom", "grp")),
        P(),
        P(),
        P(),
        P(),
        P(),
        P(),
    )
    return jax.shard_map(
        on_device, mesh=mesh, in_specs=placed, out_specs=P(("dom", "grp"), None), check_vma=False
    )
```
